32 devices in a mesh: rows: 8 (over z, y), groups: 4 (over x, core).
Axes of the slice: x: 2, y: 2, z: 4, core: 2. Of those that a mesh axis runs over, the one named last changes fastest.
Arguments:
- basis: bfloat16 [8, 131072, 128], P(None, ('rows', 'groups')), may hold values from -6 to 6
- image: bfloat16 [8, 131072, 128], P(None, ('rows', 'groups')), may hold values from -6 to 6
- selection: int32 [8, 64], replicated, may hold values from 0 to 127, all different within a row
Outputs:
- rotated: bfloat16 [8, 131072, 128], P(None, ('rows', 'groups'))
The draws below stay inside these ranges and needn't reach their ends.
Inputs may be any that keep to these rules, and one draw needn't show every extreme that they name: Each row of selection names 64 different columns.
All inputs are finite; a program needn't handle non-finite values.
Results may differ from the reference program's by a relative error of at most 0.005.
Values may be sent and summed in bfloat16 or wider, within the bound.
A program may use at most 128 MiB of HBM per device.

```python
import jax
import jax.numpy as jnp
from jax import lax

RECYCLE = 64
COLS = 128
NSYS = 8
ITERS = 3
NROWS = 131072


def levels(own_key, shape, shards, smallest, largest):
    gain = 1.0
    for position, shards_of in shards:
        steps = jax.random.uniform(jax.random.fold_in(jax.random.fold_in(own_key, 6), position), (shards_of,), jnp.float32, smallest / len(shards), largest / len(shards))
        gain = gain * jnp.repeat(jnp.exp(steps), shape[position] // shards_of).reshape((-1,) + (1,) * (len(shape) - 1 - position))
    return gain


def picks_of(rng, rows, amount, top, lift):
    sequence = jax.random.permutation(jax.random.fold_in(rng, 1), amount)
    favour = sequence
    for power in range(3):
        favour = favour * favour // amount
    favour = favour * lift // amount
    chance = jax.random.randint(jax.random.fold_in(rng, 2), (rows, amount), 0, 4096) + favour
    sure = jax.random.permutation(jax.random.fold_in(rng, 3), rows)[jnp.arange(amount) % rows]
    chance = jnp.where(jnp.arange(rows)[:, None] == sure[None, :], 1 << 14, chance)
    merit = chance * amount + jnp.arange(amount)
    return lax.top_k(merit.astype(jnp.int32), top)[1].astype(jnp.int32)


def noise(key, dims, scale, limit, split=(), kind=jnp.bfloat16):
    gain = levels(key, dims, split, -0.22, 0.18) if split else 1.0
    values = jax.random.normal(key, dims, jnp.float32) * scale * gain
    return jnp.minimum(jnp.maximum(values, -limit), limit).astype(kind)


def setup_inputs(seed: int = 0) -> dict:
    streams_of = jax.random.split(jax.random.key(seed), 4)
    basis = noise(streams_of[0], (NSYS, NROWS, COLS), 1.0, 6.0, ((1, 32),))
    image = noise(streams_of[1], (NSYS, NROWS, COLS), 1.0, 6.0, ((1, 32),))
    selection = picks_of(streams_of[2], NSYS, COLS, RECYCLE, 0)
    return dict(basis=basis, image=image, selection=selection)


def small_solve(grams, chosen):
    gram_s, cross, gram_f = (grams[0], grams[1], grams[2])
    width = gram_s.shape[0]
    coeffs = (jnp.arange(width, dtype=jnp.int32)[:, None] == chosen[None, :]).astype(jnp.float32)
    factor = jnp.linalg.cholesky(gram_f)
    for step in range(ITERS):
        moved = jnp.dot(cross.T, coeffs, precision=lax.Precision.HIGHEST)
        halfway = lax.linalg.triangular_solve(factor, moved, left_side=True, lower=True)
        solved = lax.linalg.triangular_solve(factor, halfway, left_side=True, lower=True, transpose_a=True)
        metric = jnp.dot(solved.T, jnp.dot(gram_s, solved, precision=lax.Precision.HIGHEST), precision=lax.Precision.HIGHEST) / NROWS
        lower = jnp.linalg.cholesky(metric)
        coeffs = lax.linalg.triangular_solve(lower, solved, left_side=False, lower=True, transpose_a=True)
    return coeffs

def one_system(items):
    left, right, chosen = items
    gram_s = jnp.dot(left.T.astype(jnp.float32), left.astype(jnp.float32), preferred_element_type=jnp.float32)
    cross = jnp.dot(left.T.astype(jnp.float32), right.astype(jnp.float32), preferred_element_type=jnp.float32)
    gram_f = jnp.dot(right.T.astype(jnp.float32), right.astype(jnp.float32), preferred_element_type=jnp.float32)
    coeffs = small_solve(jnp.stack([gram_s, cross, gram_f]), chosen).astype(jnp.bfloat16)
    first = jnp.dot(left.astype(jnp.float32), coeffs.astype(jnp.float32), preferred_element_type=jnp.float32)
    second = jnp.dot(right.astype(jnp.float32), coeffs.astype(jnp.float32), preferred_element_type=jnp.float32)
    return jnp.concatenate([first, second], axis=1).astype(jnp.bfloat16)

def reference(basis, image, selection):
    return lax.map(one_system, (basis, image, selection))
```

```python
import functools

import jax
import jax.numpy as jnp
from jax import lax
from jax.experimental import pallas as pl
from jax.experimental.pallas import tpu as pltpu
from jax.sharding import PartitionSpec as P

ITERS = 3
PANEL = 8
MESH = pl.DeviceIdType.MESH
NT = (((1,), (1,)), ((), ()))
TN = (((0,), (0,)), ((), ()))
HIGHEST = lax.Precision.HIGHEST


def exact_dot(a, b, dims=(((1,), (0,)), ((), ()))):
    return lax.dot_general(a, b, dims, precision=HIGHEST, preferred_element_type=jnp.float32)


def panel_rows(rows, first, forward):
    lanes = rows.shape[1]
    place = lax.broadcasted_iota(jnp.int32, (PANEL, 128), 0)
    wide = lax.broadcasted_iota(jnp.int32, (PANEL, lanes), 0)
    cols = [
        jnp.broadcast_to(rows[:, first + k : first + k + 1], (PANEL, 128)) for k in range(PANEL)
    ]
    full = rows
    lower = rows
    scales = []
    for j in range(PANEL):
        pivot = jnp.broadcast_to(cols[j][j : j + 1, :], (PANEL, 128))
        inv = 1.0 / pivot
        inv_wide = jnp.concatenate([inv] * (lanes // 128), axis=1)
        col_wide = jnp.concatenate([cols[j]] * (lanes // 128), axis=1)
        unit = jnp.broadcast_to(full[j : j + 1, :], full.shape) * inv_wide
        if forward:
            step = jnp.broadcast_to(lower[j : j + 1, :], lower.shape) * inv_wide
            lower = jnp.where(wide > j, lower - col_wide * step, lower)
            scales.append(pivot)
        full = jnp.where(wide == j, unit, full - col_wide * unit)
        for k in range(j + 1, PANEL):
            part = jnp.broadcast_to(cols[k][j : j + 1, :], (PANEL, 128)) * inv
            cols[k] = jnp.where(place == j, part, cols[k] - cols[j] * part)
    if not forward:
        return full, None
    pivots = scales[0]
    for j in range(1, PANEL):
        pivots = jnp.where(place == j, scales[j], pivots)
    root = lax.rsqrt(pivots)
    return full, lower * jnp.concatenate([root] * (lanes // 128), axis=1)


def solve_spd(work):
    n, lanes = work.shape
    for p in range(n // PANEL):
        first = p * PANEL
        full, _ = panel_rows(work[first : first + PANEL], first, False)
        moved = work
        for k in range(PANEL):
            moved = moved - work[:, first + k : first + k + 1] * full[k : k + 1, :]
        pieces = [moved[:first], full, moved[first + PANEL :]]
        work = jnp.concatenate([x for x in pieces if x.shape[0]], axis=0)
    return work[:, 128:]


def whiten(work):
    n, lanes = work.shape
    out = []
    for p in range(n // PANEL):
        first = p * PANEL
        full, lower = panel_rows(work[:PANEL], first, True)
        out.append(lower[:, 128:])
        work = work[PANEL:]
        if work.shape[0]:
            moved = work
            for k in range(PANEL):
                moved = moved - work[:, first + k : first + k + 1] * full[k : k + 1, :]
            work = moved
    return jnp.concatenate(out, axis=0)


def small_solve(gram_s, cross, gram_f, start, total_rows):
    width = gram_s.shape[0]
    keep = start.shape[0]
    across = solve_spd(jnp.concatenate([gram_f, cross.T], axis=1))
    turned = across.T
    coeffs = start
    for step in range(ITERS):
        solved = exact_dot(coeffs, turned)
        metric = exact_dot(exact_dot(solved, gram_s), solved, NT) / total_rows
        pad = jnp.zeros((keep, 128 - keep), jnp.float32)
        coeffs = whiten(jnp.concatenate([metric, pad, solved], axis=1))
    return coeffs


def pack(gram, width):
    gram_s = gram[:width, :width]
    gram_f = gram[width:, width:]
    row = lax.broadcasted_iota(jnp.int32, (width, width), 0)
    col = lax.broadcasted_iota(jnp.int32, (width, width), 1)
    mixed = jnp.where(row < col, gram_s, gram_f)
    diag = jnp.sum(jnp.where(row == col, gram_s, 0.0), axis=0, keepdims=True)
    return gram[:width, width:], mixed, jnp.broadcast_to(diag, (8, width))


def unpack(packed, width):
    cross = packed[:width]
    mixed = packed[width : 2 * width]
    diag = packed[2 * width : 2 * width + 1]
    row = lax.broadcasted_iota(jnp.int32, (width, width), 0)
    col = lax.broadcasted_iota(jnp.int32, (width, width), 1)
    turned = mixed.T
    gram_s = jnp.where(row < col, mixed, jnp.where(row > col, turned, diag))
    gram_f = jnp.where(row < col, turned, mixed)
    return gram_s, cross, gram_f


def coeff_kernel(
    sizes, total_rows, basis, image, chosen, out, shared, grams, got1, got2, got3, got4, sends, recvs, csend, crecv
):
    n_rows, n_groups = sizes
    nsys = grams.shape[0]
    width = basis.shape[2]
    inner = nsys // n_groups
    depth = n_rows // inner
    n_x = n_groups // 2
    step = pl.program_id(0)
    me_r = lax.axis_index("rows")
    me_g = lax.axis_index("groups")
    z, y = me_r // inner, lax.rem(me_r, inner)
    x, c = me_g // 2, lax.rem(me_g, 2)
    barrier = pltpu.get_barrier_semaphore()
    peers = n_rows * n_groups

    def nth_peer(i):
        other = lax.rem(me_r * n_groups + me_g + i, peers)
        return (other // n_groups, lax.rem(other, n_groups))

    @pl.when(step == 0)
    def _():
        def greet(i, carry):
            pl.semaphore_signal(barrier, inc=1, device_id=nth_peer(i), device_id_type=MESH)
            return carry

        lax.fori_loop(1, peers, greet, 0)

    both = jnp.concatenate([basis[0], image[0]], axis=1)
    gram = lax.dot_general(both, both, TN, preferred_element_type=jnp.float32)
    cross, mixed, diag = pack(gram, width)
    grams[step, 0:width, :] = cross
    grams[step, width : 2 * width, :] = mixed
    grams[step, 2 * width :, :] = diag

    @pl.when(step == nsys - 1)
    def _():
        pl.semaphore_wait(barrier, peers - 1)
        base = 0
        count = nsys
        slot = 0
        for size, at, spot, got in (
            (2, c, lambda k: (me_r, me_g + k - c), got1),
            (n_x, x, lambda k: (me_r, me_g + 2 * (k - x)), got2),
            (inner, y, lambda k: (me_r + k - y, me_g), got3),
        ):
            if size == 1:
                continue
            count = count // size
            copies = []
            for d in range(1, size):
                k = lax.rem(at + d, size)
                copy = pltpu.make_async_remote_copy(
                    src_ref=grams.at[pl.ds(base + k * count, count)],
                    dst_ref=got.at[pl.ds((d - 1) * count, count)],
                    send_sem=sends.at[slot],
                    recv_sem=recvs.at[slot],
                    device_id=spot(k),
                    device_id_type=MESH,
                )
                copy.start()
                copies.append(copy)
                slot += 1
            base = base + at * count
            for d, copy in enumerate(copies):
                copy.wait()
                grams[pl.ds(base, count)] += got[pl.ds(d * count, count)]
        mine = base
        root = lax.rem(2 * c + x + y, depth)

        @pl.when(z != root)
        def _():
            copy = pltpu.make_async_remote_copy(
                src_ref=grams.at[mine],
                dst_ref=got4.at[lax.rem(z - root + depth, depth) - 1],
                send_sem=sends.at[slot],
                recv_sem=recvs.at[slot + lax.rem(z - root + depth, depth) - 1],
                device_id=(root * inner + y, me_g),
                device_id_type=MESH,
            )
            copy.start()
            copy.wait_send()

        @pl.when(z == root)
        def _():
            total = grams[mine]
            for k in range(depth - 1):
                pltpu.make_async_remote_copy(
                    src_ref=grams.at[mine],
                    dst_ref=got4.at[k],
                    send_sem=sends.at[slot],
                    recv_sem=recvs.at[slot + k],
                    device_id=(me_r, me_g),
                    device_id_type=MESH,
                ).wait_recv()
                total = total + got4[k]
            gram_s, cross_s, gram_f = unpack(total, width)
            picked = chosen[pl.ds(mine, 1), :]
            row = lax.broadcasted_iota(jnp.int32, (width, picked.shape[1]), 0)
            start = (row == picked).astype(jnp.float32).T
            coeffs = small_solve(gram_s, cross_s, gram_f, start, total_rows)
            shared[pl.ds(mine, 1)] = coeffs.astype(jnp.bfloat16)[None]

            def share(i):
                return pltpu.make_async_remote_copy(
                    src_ref=shared.at[mine],
                    dst_ref=shared.at[mine],
                    send_sem=csend.at[i],
                    recv_sem=crecv.at[mine],
                    device_id=nth_peer(i),
                    device_id_type=MESH,
                )

            def send(i, carry):
                share(i).start()
                return carry

            def sent(i, carry):
                share(i).wait_send()
                return carry

            lax.fori_loop(1, peers, send, 0)
            lax.fori_loop(1, peers, sent, 0)

        for s in range(nsys):

            @pl.when(jnp.logical_or(z != root, mine != s))
            def _():
                pltpu.make_async_remote_copy(
                    src_ref=shared.at[s],
                    dst_ref=shared.at[s],
                    send_sem=csend.at[0],
                    recv_sem=crecv.at[s],
                    device_id=(me_r, me_g),
                    device_id_type=MESH,
                ).wait_recv()

        out[...] = shared[...]


def rotate_kernel(basis, image, coeffs, out):
    narrow = coeffs[0]
    first = lax.dot_general(basis[0], narrow, NT, preferred_element_type=jnp.float32)
    second = lax.dot_general(image[0], narrow, NT, preferred_element_type=jnp.float32)
    out[0] = jnp.concatenate([first, second], axis=1).astype(out.dtype)


def on_device(n_rows, n_groups, basis, image, selection):
    nsys, local, width = basis.shape
    keep = selection.shape[1]
    peers = n_rows * n_groups
    total_rows = local * peers
    inner = nsys // n_groups
    depth = n_rows // inner
    n_x = n_groups // 2
    hops = n_x + max(inner - 1, 1)
    tall = 2 * width + 8
    whole = pl.BlockSpec((1, local, width), lambda s: (s, 0, 0))
    coeffs = pl.pallas_call(
        functools.partial(coeff_kernel, (n_rows, n_groups), total_rows),
        grid=(nsys,),
        in_specs=[whole, whole, pl.BlockSpec(memory_space=pltpu.VMEM)],
        out_specs=pl.BlockSpec(memory_space=pltpu.VMEM),
        out_shape=jax.ShapeDtypeStruct((nsys, keep, width), jnp.bfloat16),
        scratch_shapes=[
            pltpu.VMEM((nsys, keep, width), jnp.bfloat16),
            pltpu.VMEM((nsys, tall, width), jnp.float32),
            pltpu.VMEM((nsys // 2, tall, width), jnp.float32),
            pltpu.VMEM(((n_x - 1) * nsys // n_groups, tall, width), jnp.float32),
            pltpu.VMEM((max(inner - 1, 1), tall, width), jnp.float32),
            pltpu.VMEM((depth - 1, tall, width), jnp.float32),
            pltpu.SemaphoreType.DMA((hops + 1,)),
            pltpu.SemaphoreType.DMA((hops + depth - 1,)),
            pltpu.SemaphoreType.DMA((peers,)),
            pltpu.SemaphoreType.DMA((nsys,)),
        ],
        compiler_params=pltpu.CompilerParams(
            collective_id=0, has_side_effects=True, dimension_semantics=("arbitrary",)
        ),
    )(basis, image, selection)
    return pl.pallas_call(
        rotate_kernel,
        grid=(nsys,),
        in_specs=[whole, whole, pl.BlockSpec((1, keep, width), lambda s: (s, 0, 0))],
        out_specs=whole,
        out_shape=jax.ShapeDtypeStruct((nsys, local, width), jnp.bfloat16),
    )(basis, image, coeffs)


def solution(mesh):
    in_specs = (P(None, ("rows", "groups"), None), P(None, ("rows", "groups"), None), P())
    out_specs = P(None, ("rows", "groups"), None)
    return jax.shard_map(
        functools.partial(on_device, mesh.shape["rows"], mesh.shape["groups"]),
        mesh=mesh,
        in_specs=in_specs,
        out_specs=out_specs,
        check_vma=False,
    )
```

```python
import functools

import jax
import jax.numpy as jnp
from jax import lax
from jax.experimental import pallas as pl
from jax.experimental.pallas import tpu as pltpu
from jax.sharding import PartitionSpec as P

ITERS = 3
PANEL = 8
MESH = pl.DeviceIdType.MESH
NT = (((1,), (1,)), ((), ()))
TN = (((0,), (0,)), ((), ()))
HIGHEST = lax.Precision.HIGHEST


def exact_dot(a, b, dims=(((1,), (0,)), ((), ()))):
    return lax.dot_general(a, b, dims, precision=HIGHEST, preferred_element_type=jnp.float32)


def panel_rows(rows, first, forward):
    lanes = rows.shape[1]
    place = lax.broadcasted_iota(jnp.int32, (PANEL, 128), 0)
    wide = lax.broadcasted_iota(jnp.int32, (PANEL, lanes), 0)
    cols = [
        jnp.broadcast_to(rows[:, first + k : first + k + 1], (PANEL, 128)) for k in range(PANEL)
    ]
    full = rows
    lower = rows
    scales = []
    for j in range(PANEL):
        pivot = jnp.broadcast_to(cols[j][j : j + 1, :], (PANEL, 128))
        inv = 1.0 / pivot
        inv_wide = jnp.concatenate([inv] * (lanes // 128), axis=1)
        col_wide = jnp.concatenate([cols[j]] * (lanes // 128), axis=1)
        unit = jnp.broadcast_to(full[j : j + 1, :], full.shape) * inv_wide
        if forward:
            step = jnp.broadcast_to(lower[j : j + 1, :], lower.shape) * inv_wide
            lower = jnp.where(wide > j, lower - col_wide * step, lower)
            scales.append(pivot)
        full = jnp.where(wide == j, unit, full - col_wide * unit)
        for k in range(j + 1, PANEL):
            part = jnp.broadcast_to(cols[k][j : j + 1, :], (PANEL, 128)) * inv
            cols[k] = jnp.where(place == j, part, cols[k] - cols[j] * part)
    if not forward:
        return full, None
    pivots = scales[0]
    for j in range(1, PANEL):
        pivots = jnp.where(place == j, scales[j], pivots)
    root = lax.rsqrt(pivots)
    return full, lower * jnp.concatenate([root] * (lanes // 128), axis=1)


def solve_spd(work):
    n, lanes = work.shape
    for p in range(n // PANEL):
        first = p * PANEL
        full, _ = panel_rows(work[first : first + PANEL], first, False)
        moved = work
        for k in range(PANEL):
            moved = moved - work[:, first + k : first + k + 1] * full[k : k + 1, :]
        pieces = [moved[:first], full, moved[first + PANEL :]]
        work = jnp.concatenate([x for x in pieces if x.shape[0]], axis=0)
    return work[:, 128:]


def whiten(work):
    n, lanes = work.shape
    out = []
    for p in range(n // PANEL):
        first = p * PANEL
        full, lower = panel_rows(work[:PANEL], first, True)
        out.append(lower[:, 128:])
        work = work[PANEL:]
        if work.shape[0]:
            moved = work
            for k in range(PANEL):
                moved = moved - work[:, first + k : first + k + 1] * full[k : k + 1, :]
            work = moved
    return jnp.concatenate(out, axis=0)


def small_solve(gram_s, cross, gram_f, start, total_rows):
    width = gram_s.shape[0]
    keep = start.shape[0]
    across = solve_spd(jnp.concatenate([gram_f, cross.T], axis=1))
    turned = across.T
    coeffs = start
    for step in range(ITERS):
        solved = exact_dot(coeffs, turned)
        metric = exact_dot(exact_dot(solved, gram_s), solved, NT) / total_rows
        pad = jnp.zeros((keep, 128 - keep), jnp.float32)
        coeffs = whiten(jnp.concatenate([metric, pad, solved], axis=1))
    return coeffs


def pack(gram, width):
    gram_s = gram[:width, :width]
    gram_f = gram[width:, width:]
    row = lax.broadcasted_iota(jnp.int32, (width, width), 0)
    col = lax.broadcasted_iota(jnp.int32, (width, width), 1)
    mixed = jnp.where(row < col, gram_s, gram_f)
    diag = jnp.sum(jnp.where(row == col, gram_s, 0.0), axis=0, keepdims=True)
    return gram[:width, width:], mixed, jnp.broadcast_to(diag, (8, width))


def unpack(packed, width):
    cross = packed[:width]
    mixed = packed[width : 2 * width]
    diag = packed[2 * width : 2 * width + 1]
    row = lax.broadcasted_iota(jnp.int32, (width, width), 0)
    col = lax.broadcasted_iota(jnp.int32, (width, width), 1)
    turned = mixed.T
    gram_s = jnp.where(row < col, mixed, jnp.where(row > col, turned, diag))
    gram_f = jnp.where(row < col, turned, mixed)
    return gram_s, cross, gram_f


def place_of(nsys, n_rows, n_groups):
    inner = nsys // n_groups
    me_r = lax.axis_index("rows")
    me_g = lax.axis_index("groups")
    return me_r // inner, lax.rem(me_r, inner), me_g // 2, lax.rem(me_g, 2)


def system_at(nsys, n_rows, n_groups, step):
    half, inner, n_x = nsys // 2, nsys // n_groups, n_groups // 2
    z, y, x, c = place_of(nsys, n_rows, n_groups)
    rest = lax.rem(step, half)
    core = lax.rem(c + 1 - step // half, 2)
    along = lax.rem(x + n_x - 1 - rest // inner, n_x)
    row = lax.rem(y + inner - 1 - lax.rem(rest, inner), inner)
    return core * half + along * inner + row


def coeff_kernel(
    sizes, total_rows, basis, image, chosen, out, shared, grams, got1, got2, got3, got4,
    send1, recv1, send2, recv2, send3, recv3, send4, recv4, csend, crecv
):
    n_rows, n_groups = sizes
    nsys = grams.shape[0]
    width = basis.shape[2]
    half, inner, n_x = nsys // 2, nsys // n_groups, n_groups // 2
    depth = n_rows // inner
    late = min(2, half - 1)
    step = pl.program_id(0)
    me_r = lax.axis_index("rows")
    me_g = lax.axis_index("groups")
    z, y, x, c = place_of(nsys, n_rows, n_groups)
    barrier = pltpu.get_barrier_semaphore()
    peers = n_rows * n_groups

    def at(t):
        return system_at(nsys, n_rows, n_groups, t)

    def nth_peer(i):
        other = lax.rem(me_r * n_groups + me_g + i, peers)
        return (other // n_groups, lax.rem(other, n_groups))

    def to_core(t):
        spot = lax.rem(at(t), half)
        return pltpu.make_async_remote_copy(
            src_ref=grams.at[at(t)],
            dst_ref=got1.at[spot],
            send_sem=send1.at[spot],
            recv_sem=recv1.at[spot],
            device_id=(me_r, me_g + 1 - 2 * c),
            device_id_type=MESH,
        )

    def along_x(dx, dy):
        spot = (dx - 1) * inner + lax.rem(y + dy, inner)
        k = lax.rem(x + dx, n_x)
        return pltpu.make_async_remote_copy(
            src_ref=grams.at[c * half + k * inner + lax.rem(y + dy, inner)],
            dst_ref=got2.at[spot],
            send_sem=send2.at[spot],
            recv_sem=recv2.at[spot],
            device_id=(me_r, k * 2 + c),
            device_id_type=MESH,
        )

    def along_rows(dy):
        k = lax.rem(y + dy, inner)
        return pltpu.make_async_remote_copy(
            src_ref=grams.at[c * half + x * inner + k],
            dst_ref=got3.at[dy - 1],
            send_sem=send3.at[dy - 1],
            recv_sem=recv3.at[dy - 1],
            device_id=(z * inner + k, me_g),
            device_id_type=MESH,
        )

    @pl.when(step == 0)
    def _():
        def greet(i, carry):
            pl.semaphore_signal(barrier, inc=1, device_id=nth_peer(i), device_id_type=MESH)
            return carry

        lax.fori_loop(1, peers, greet, 0)

    both = jnp.concatenate([basis[0], image[0]], axis=1)
    gram = lax.dot_general(both, both, TN, preferred_element_type=jnp.float32)
    cross, mixed, diag = pack(gram, width)
    now = at(step)
    grams[now, 0:width, :] = cross
    grams[now, width : 2 * width, :] = mixed
    grams[now, 2 * width :, :] = diag

    @pl.when(step == late)
    def _():
        pl.semaphore_wait(barrier, peers - 1)
        for t in range(late + 1):
            to_core(t).start()

    @pl.when(jnp.logical_and(step > late, step < half))
    def _():
        to_core(step).start()

    for t in range(half, nsys):

        @pl.when(step == t)
        def _():
            own = at(t)
            spot = lax.rem(own, half)
            to_core(t).wait_recv()
            grams[own] += got1[spot]
            dx = n_x - 1 - (t - half) // inner
            if dx:
                along_x(dx, inner - 1 - (t - half) % inner).start()

    @pl.when(step == nsys - 1)
    def _():
        base = c * half + x * inner
        for dy in reversed(range(inner)):
            k = lax.rem(y + dy, inner)
            for dx in range(1, n_x):
                along_x(dx, dy).wait_recv()
                grams[base + k] += got2[(dx - 1) * inner + k]
            if dy:
                along_rows(dy).start()
        mine = base + y
        for dy in range(1, inner):
            along_rows(dy).wait_recv()
            grams[mine] += got3[dy - 1]
        root = lax.rem(2 * c + x + y, depth)

        @pl.when(z != root)
        def _():
            copy = pltpu.make_async_remote_copy(
                src_ref=grams.at[mine],
                dst_ref=got4.at[lax.rem(z - root + depth, depth) - 1],
                send_sem=send4.at[0],
                recv_sem=recv4.at[lax.rem(z - root + depth, depth) - 1],
                device_id=(root * inner + y, me_g),
                device_id_type=MESH,
            )
            copy.start()
            copy.wait_send()

        @pl.when(z == root)
        def _():
            total = grams[mine]
            for k in range(depth - 1):
                pltpu.make_async_remote_copy(
                    src_ref=grams.at[mine],
                    dst_ref=got4.at[k],
                    send_sem=send4.at[0],
                    recv_sem=recv4.at[k],
                    device_id=(me_r, me_g),
                    device_id_type=MESH,
                ).wait_recv()
                total = total + got4[k]
            gram_s, cross_s, gram_f = unpack(total, width)
            picked = chosen[pl.ds(mine, 1), :]
            row = lax.broadcasted_iota(jnp.int32, (width, picked.shape[1]), 0)
            start = (row == picked).astype(jnp.float32).T
            coeffs = small_solve(gram_s, cross_s, gram_f, start, total_rows)
            shared[pl.ds(mine, 1)] = coeffs.astype(jnp.bfloat16)[None]

            def share(i):
                return pltpu.make_async_remote_copy(
                    src_ref=shared.at[mine],
                    dst_ref=shared.at[mine],
                    send_sem=csend.at[i],
                    recv_sem=crecv.at[mine],
                    device_id=nth_peer(i),
                    device_id_type=MESH,
                )

            def send(i, carry):
                share(i).start()
                return carry

            def sent(i, carry):
                share(i).wait_send()
                return carry

            lax.fori_loop(1, peers, send, 0)
            lax.fori_loop(1, peers, sent, 0)

        for s in range(nsys):

            @pl.when(jnp.logical_or(z != root, mine != s))
            def _():
                pltpu.make_async_remote_copy(
                    src_ref=shared.at[s],
                    dst_ref=shared.at[s],
                    send_sem=csend.at[0],
                    recv_sem=crecv.at[s],
                    device_id=(me_r, me_g),
                    device_id_type=MESH,
                ).wait_recv()

        for t in range(half):
            to_core(t).wait_send()
        for dy in range(inner):
            for dx in range(1, n_x):
                along_x(dx, dy).wait_send()
            if dy:
                along_rows(dy).wait_send()
        out[...] = shared[...]


def rotate_kernel(basis, image, coeffs, out):
    narrow = coeffs[0]
    empty = jnp.zeros_like(narrow)
    upper = jnp.concatenate([narrow, empty], axis=1)
    lower = jnp.concatenate([empty, narrow], axis=1)
    both = jnp.concatenate([basis[0], image[0]], axis=1)
    twice = jnp.concatenate([upper, lower], axis=0)
    turned = lax.dot_general(both, twice, NT, preferred_element_type=jnp.float32)
    out[0] = turned.astype(out.dtype)


def on_device(n_rows, n_groups, basis, image, selection):
    nsys, local, width = basis.shape
    keep = selection.shape[1]
    peers = n_rows * n_groups
    total_rows = local * peers
    inner = nsys // n_groups
    depth = n_rows // inner
    n_x = n_groups // 2
    tall = 2 * width + 8
    whole = pl.BlockSpec((1, local, width), lambda s: (s, 0, 0))
    ordered = pl.BlockSpec(
        (1, local, width), lambda s: (system_at(nsys, n_rows, n_groups, s), 0, 0)
    )
    coeffs = pl.pallas_call(
        functools.partial(coeff_kernel, (n_rows, n_groups), total_rows),
        grid=(nsys,),
        in_specs=[ordered, ordered, pl.BlockSpec(memory_space=pltpu.VMEM)],
        out_specs=pl.BlockSpec(memory_space=pltpu.VMEM),
        out_shape=jax.ShapeDtypeStruct((nsys, keep, width), jnp.bfloat16),
        scratch_shapes=[
            pltpu.VMEM((nsys, keep, width), jnp.bfloat16),
            pltpu.VMEM((nsys, tall, width), jnp.float32),
            pltpu.VMEM((nsys // 2, tall, width), jnp.float32),
            pltpu.VMEM(((n_x - 1) * nsys // n_groups, tall, width), jnp.float32),
            pltpu.VMEM((max(inner - 1, 1), tall, width), jnp.float32),
            pltpu.VMEM((depth - 1, tall, width), jnp.float32),
            pltpu.SemaphoreType.DMA((nsys // 2,)),
            pltpu.SemaphoreType.DMA((nsys // 2,)),
            pltpu.SemaphoreType.DMA(((n_x - 1) * inner,)),
            pltpu.SemaphoreType.DMA(((n_x - 1) * inner,)),
            pltpu.SemaphoreType.DMA((max(inner - 1, 1),)),
            pltpu.SemaphoreType.DMA((max(inner - 1, 1),)),
            pltpu.SemaphoreType.DMA((1,)),
            pltpu.SemaphoreType.DMA((depth - 1,)),
            pltpu.SemaphoreType.DMA((peers,)),
            pltpu.SemaphoreType.DMA((nsys,)),
        ],
        compiler_params=pltpu.CompilerParams(
            collective_id=0, has_side_effects=True, dimension_semantics=("arbitrary",)
        ),
    )(basis, image, selection)
    return pl.pallas_call(
        rotate_kernel,
        grid=(nsys,),
        in_specs=[whole, whole, pl.BlockSpec((1, keep, width), lambda s: (s, 0, 0))],
        out_specs=whole,
        out_shape=jax.ShapeDtypeStruct((nsys, local, width), jnp.bfloat16),
    )(basis, image, coeffs)


def solution(mesh):
    in_specs = (P(None, ("rows", "groups"), None), P(None, ("rows", "groups"), None), P())
    out_specs = P(None, ("rows", "groups"), None)
    return jax.shard_map(
        functools.partial(on_device, mesh.shape["rows"], mesh.shape["groups"]),
        mesh=mesh,
        in_specs=in_specs,
        out_specs=out_specs,
        check_vma=False,
    )
```
